32 devices in a mesh: row: 8 (over y, x, core), col: 4 (over z).
Axes of the slice: x: 2, y: 2, z: 4, core: 2. Of those that a mesh axis runs over, the one named last changes fastest.
Arguments:
- singular_vectors: float32 [4096, 4096], P('row', 'col'), may hold values from -6 to 6
- reflector_vectors: float32 [2, 16, 256, 512], P(None, 'row', 'col'), may hold values from -2 to 2, as said below
- reflector_factors: float32 [2, 16, 256, 256], P(None, 'row', 'col'), as said below
- sweep_bounds: int32 [2, 2], replicated, may hold values from 0 to 3584, as said below
Outputs:
- transformed: float32 [4096, 4096], P('row', 'col')
The draws below stay inside these ranges and needn't reach their ends.
Inputs may be any that keep to these rules, and one draw needn't show every extreme that they name: `reflector_vectors`: row j of each block's 256 x 2 * 256 slice is a reflector: 1 at position j, nonzero only at positions j to j + 255. `reflector_factors`: each block's factor is the upper triangular inverse of the strictly upper part of W W^T plus half of its diagonal, W being that block's slice of reflector_vectors, so that each block's transformation is orthogonal. `sweep_bounds`: both entries are multiples of 256, and the first is below the second.
All inputs are finite; a program needn't handle non-finite values.
Results may differ from the reference program's by a relative error of at most 0.0003.
Values sent between devices are 32-bit elements; how exact they have to be, the bound alone decides.
No kernel may reach another device: no remote copies, remote signals or barrier semaphores. Data moves between devices by JAX's collectives and lax.ppermute only.
A program may use at most 64 MiB of HBM per device.

```python
import jax
import jax.numpy as jnp
from jax import lax

BW = 256
NV = 4096
SWEEPS = 2
ROWS = 4096
BLOCKS = 16


exact_mode = lax.Precision.HIGHEST


def build_factor(vectors):
    gram = jnp.dot(vectors, vectors.T, precision=exact_mode, preferred_element_type=jnp.float32)
    upper = jnp.triu(gram, 1) + jnp.diag(0.5 * jnp.diagonal(gram))
    identity = jnp.eye(gram.shape[0], dtype=jnp.float32)
    return lax.linalg.triangular_solve(upper, identity, left_side=True, lower=False)


def reflector_pair(key):
    base_key = jax.random.fold_in(key, 11)
    tail_scale = 0.25 / BW ** 0.5
    noise = jax.random.truncated_normal(base_key, -4.0, 4.0, (SWEEPS, BLOCKS, BW, 2 * BW), jnp.float32)
    column = lax.broadcasted_iota(jnp.int32, (BW, 2 * BW), 1)
    reflector_row = lax.broadcasted_iota(jnp.int32, (BW, 2 * BW), 0)
    tail_mask = (column > reflector_row) & (column < reflector_row + BW)
    head_mask = column == reflector_row
    far_mask = column == reflector_row + BW - 1
    vectors = jnp.where(tail_mask, noise * tail_scale, 0.0) + jnp.where(head_mask, 1.0, 0.0) + jnp.where(far_mask, 1.0, 0.0)
    vectors = vectors.astype(jnp.float32)
    factors = jax.vmap(jax.vmap(build_factor))(vectors)
    return (vectors, factors)


def draw_reflector_vectors(key, part):
    return reflector_pair(key)[0]


def draw_reflector_factors(key, part):
    return reflector_pair(key)[1]


def draw_sweep_bounds(key, part):
    first_key = jax.random.fold_in(key, 21)
    last_key = jax.random.fold_in(key, 22)
    first_row = jax.random.randint(first_key, (SWEEPS,), 0, BLOCKS // 4) * BW
    last_row = jax.random.randint(last_key, (SWEEPS,), BLOCKS * 3 // 4 - 1, BLOCKS - 1) * BW
    return jnp.stack([first_row, last_row], axis=1).astype(jnp.int32)


def steps_of(own_key, dims, pieces, smallest, largest):
    level, own = 1.0, jax.random.fold_in(own_key, 6)
    for axis_at, shards_of in pieces:
        heights = jnp.exp(jax.random.uniform(jax.random.fold_in(own, axis_at), (shards_of,), jnp.float32, smallest / len(pieces), largest / len(pieces)))
        level = level * jnp.repeat(heights, dims[axis_at] // shards_of).reshape([-1 if axis == axis_at else 1 for axis in range(len(dims))])
    return level


def centred(stream_key, shape, deviation, most, pieces=(), held_as=jnp.bfloat16):
    array = jax.random.normal(stream_key, shape, jnp.float32) * deviation
    if len(pieces) > 0:
        array = steps_of(stream_key, shape, pieces, -0.22, 0.18) * array
    return jnp.clip(array, min=-most, max=most).astype(held_as)


def setup_inputs(seed: int = 0) -> dict:
    arg_keys = jax.random.split(jax.random.key(seed), 5)
    return {
        "singular_vectors": centred(arg_keys[0], (ROWS, NV), 1.0, 6.0, ((0, 8), (1, 4)), jnp.float32),
        "reflector_vectors": draw_reflector_vectors(jax.random.fold_in(arg_keys[4], 71), 0),
        "reflector_factors": draw_reflector_factors(jax.random.fold_in(arg_keys[4], 71), 0),
        "sweep_bounds": draw_sweep_bounds(jax.random.fold_in(arg_keys[4], 71), 0),
    }


exact_mode = lax.Precision.HIGHEST

def apply_block(row_block, vectors, factor):
    inner_part = jnp.dot(vectors.astype(jnp.float32), row_block.astype(jnp.float32), precision=exact_mode, preferred_element_type=jnp.float32)
    inner_part = jnp.dot(factor.astype(jnp.float32), inner_part.astype(jnp.float32), precision=exact_mode, preferred_element_type=jnp.float32)
    return row_block - jnp.dot(vectors.T.astype(jnp.float32), inner_part.astype(jnp.float32), precision=exact_mode, preferred_element_type=jnp.float32)

def keep_same(matrix):
    return matrix

def reference(singular_vectors, reflector_vectors, reflector_factors, sweep_bounds):

    def one_sweep(field_now, sweep_id):
        first_row = sweep_bounds[sweep_id, 0]
        last_row = sweep_bounds[sweep_id, 1]

        def one_block(counter, current):
            block_id = (BLOCKS - 1 - counter).astype(jnp.int32)
            start_row = (block_id * BW).astype(jnp.int32)
            is_live = (start_row >= first_row) & (start_row <= last_row)

            def update(matrix):
                row_block = lax.dynamic_slice_in_dim(matrix, start_row, 2 * BW, 0)
                row_block = apply_block(row_block, reflector_vectors[sweep_id, block_id], reflector_factors[sweep_id, block_id])
                return lax.dynamic_update_slice_in_dim(matrix, row_block, start_row, 0)
            return lax.cond(is_live, update, keep_same, current)
        return (lax.fori_loop(0, BLOCKS, one_block, field_now), None)
    result_field, unused = lax.scan(one_sweep, singular_vectors, jnp.arange(SWEEPS, dtype=jnp.int32))
    return result_field
```

```python
import functools

import jax
import jax.numpy as jnp
from jax import lax
from jax.experimental import pallas as pl
from jax.experimental.pallas import tpu as pltpu
from jax.sharding import PartitionSpec as P

LAG = 2
WIDTH = 128
CORES = 2
f32, bf16 = jnp.float32, jnp.bfloat16


def split(x):
    high = x.astype(bf16)
    return high, (x - high.astype(f32)).astype(bf16)


def dot3(a, b, dims):
    (ah, al), (bh, bl) = a, b
    mm = functools.partial(
        lax.dot_general, dimension_numbers=(dims, ((), ())), preferred_element_type=f32
    )
    return mm(ah, bh) + (mm(ah, bl) + mm(al, bh))


def form_block(packed, bw):
    packed_v, factor = packed[:, :bw], packed[:, bw:]
    row = lax.broadcasted_iota(jnp.int32, (bw, bw), 0)
    col = lax.broadcasted_iota(jnp.int32, (bw, bw), 1)
    upper = jnp.where(col >= row, packed_v, 0.0)
    lower = jnp.where(col < row, packed_v, 0.0)
    v = split(jnp.concatenate([upper, lower], axis=1))
    fv = split(dot3(split(factor), v, ((1,), (0,))))
    g = dot3(v, fv, ((0,), (0,)))
    row2 = lax.broadcasted_iota(jnp.int32, (2 * bw, 2 * bw), 0)
    col2 = lax.broadcasted_iota(jnp.int32, (2 * bw, 2 * bw), 1)
    return jnp.where(row2 == col2, 1.0, 0.0) - g


def prep_kernel(sweep, count, bw, cols, *refs):
    pieces, (high_ref, low_ref, packed) = refs[: 2 * cols], refs[2 * cols :]
    core = lax.rem(lax.axis_index("row"), CORES)
    z = lax.axis_index("col")
    part = bw // cols
    local = count // CORES
    for side in range(2):
        owner = core if side == 0 else 1 - core
        for i in range(local):
            for k in range(cols):
                at = lax.rem(z - k + cols, cols) * part
                packed[pl.ds(pl.multiple_of(at, part), part), :] = pieces[side * cols + k][i]
            slot = lax.rem(owner * local + i - sweep + count, count)
            high, low = split(form_block(packed[...], bw))
            high_ref[slot] = high
            low_ref[slot] = low


def prep_extra_kernel(bw, cols, *refs):
    pieces, (high_ref, low_ref, packed) = refs[:cols], refs[cols:]
    z = lax.axis_index("col")
    part = bw // cols
    for k in range(cols):
        at = lax.rem(z - k + cols, cols) * part
        packed[pl.ds(pl.multiple_of(at, part), part), :] = pieces[k][...]
    high, low = split(form_block(packed[...], bw))
    high_ref[...] = high
    low_ref[...] = low


def apply_rows(state, piece, rows, high, low):
    current = state[piece, rows, :]
    rh, rl = split(current)
    width = current.shape[1]
    wide = jnp.dot(high, jnp.concatenate([rh, rl], axis=1), preferred_element_type=f32)
    thin = jnp.dot(low, rh, preferred_element_type=f32)
    state[piece, rows, :] = wide[:, :width] + (wide[:, width:] + thin)


def unit_kernel(step, chips, sweeps, pieces, count, bw, fresh, *refs):
    bounds, state_in, incoming = refs[:3]
    mats = refs[3 : 3 + 2 * fresh]
    rest = refs[3 + 2 * fresh :]
    if fresh == sweeps:
        extra_high, extra_low = rest[:2]
        rest = rest[2:]
    state, up, down = rest
    chip = lax.axis_index("row") // CORES
    unit = step - LAG * (chips - 1 - chip)

    def live(sweep, block):
        start = block * bw
        return (start >= bounds[sweep, 0]) & (start <= bounds[sweep, 1])

    for sweep in range(fresh):
        piece = unit - sweep * pieces

        @pl.when((piece >= 0) & (piece < pieces))
        def _():
            state[piece, (count + sweep) * bw : (count + sweep + 1) * bw, :] = incoming[...]
            for slot in reversed(range(count)):

                @pl.when(live(sweep, chip * count + slot + sweep))
                def _():
                    apply_rows(
                        state,
                        piece,
                        slice((slot + sweep) * bw, (slot + sweep + 2) * bw),
                        mats[2 * sweep][slot],
                        mats[2 * sweep + 1][slot],
                    )

            up[...] = state[piece, sweep * bw : (sweep + 1) * bw, :]
            if sweep == sweeps - 1:

                @pl.when((chip == 0) & live(sweep, 0))
                def _():
                    apply_rows(state, piece, slice(0, 2 * bw), extra_high[...], extra_low[...])

                down[...] = state[piece, count * bw : (count + sweeps) * bw, :]


def finish_kernel(first_step, chips, sweeps, pieces, count, bw, *refs):
    state, keep, give = refs[0], refs[-2], refs[-1]
    messages = refs[1:-2]
    row = lax.axis_index("row")
    chip, core = row // CORES, lax.rem(row, CORES)
    half = count * bw // CORES
    width = state.shape[2]
    for piece in range(pieces):
        lanes = slice(piece * width, (piece + 1) * width)

        def low_rows(out):
            @pl.when(chip == 0)
            def _():
                out[:, lanes] = state[piece, :half, :]

            for sender in range(chips - 1):

                @pl.when(chip == sender + 1)
                def _():
                    at = (sweeps - 1) * pieces + piece + LAG * (chips - 1 - sender) - first_step
                    out[: sweeps * bw, lanes] = messages[at][...]
                    if half > sweeps * bw:
                        out[sweeps * bw :, lanes] = state[piece, sweeps * bw : half, :]

        @pl.when(core == 0)
        def _():
            low_rows(keep)
            give[:, lanes] = state[piece, half : 2 * half, :]

        @pl.when(core == 1)
        def _():
            keep[:, lanes] = state[piece, half : 2 * half, :]
            low_rows(give)


def vmem_spec():
    return pl.BlockSpec(memory_space=pltpu.VMEM)


def call(body, outs, ins, scratch=(), aliases=None, smem=(), flops=0):
    specs = [
        pl.BlockSpec(memory_space=pltpu.SMEM) if i in smem else vmem_spec()
        for i in range(len(ins))
    ]
    return pl.pallas_call(
        body,
        out_shape=tuple(outs),
        in_specs=specs,
        out_specs=tuple(vmem_spec() for _ in outs),
        scratch_shapes=list(scratch),
        input_output_aliases=aliases or {},
        cost_estimate=pl.CostEstimate(flops=flops, bytes_accessed=0, transcendentals=0),
        compiler_params=pltpu.CompilerParams(vmem_limit_bytes=32 * 2**20),
    )(*ins)


def per_device(vectors, reflectors, factors, bounds):
    rows, cols = lax.axis_size("row"), lax.axis_size("col")
    row = lax.axis_index("row")
    core = lax.rem(row, CORES)
    chips = rows // CORES
    row_dev, col_count = vectors.shape
    sweeps, blocks_dev = reflectors.shape[:2]
    bw = reflectors.shape[3] // 2
    count = blocks_dev * CORES
    half_cols = col_count // CORES
    pieces = max(1, half_cols // WIDTH)
    width = half_cols // pieces
    assert sweeps == 2

    pair = [(i, i ^ 1) for i in range(rows)]
    packed = jnp.concatenate(
        [reflectors[..., :bw] + reflectors[..., bw:], factors], axis=-1
    )

    def gather(x):
        own = [x] + [
            lax.ppermute(x, "col", [(i, (i + k) % cols) for i in range(cols)])
            for k in range(1, cols)
        ]
        return own + [lax.ppermute(part, "row", pair) for part in own]

    def shape(*dims, dtype=f32):
        return jax.ShapeDtypeStruct(dims, dtype)

    block_flops = 3 * 2 * (bw * bw * 2 * bw + 2 * bw * bw * 2 * bw)

    def prep(sweep, parts):
        return call(
            functools.partial(prep_kernel, sweep, count, bw, cols),
            [shape(count, 2 * bw, 2 * bw, dtype=bf16)] * 2,
            parts,
            scratch=[pltpu.VMEM((bw, 2 * bw), f32)],
            flops=count * block_flops,
        )

    mats = list(prep(0, gather(packed[0])))

    own_part = lax.dynamic_slice_in_dim(vectors, core * half_cols, half_cols, 1)
    other_part = lax.ppermute(
        lax.dynamic_slice_in_dim(vectors, (1 - core) * half_cols, half_cols, 1), "row", pair
    )
    is_low = core == 0
    state = jnp.concatenate(
        [
            jnp.where(is_low, own_part, other_part),
            jnp.where(is_low, other_part, own_part),
            jnp.zeros((sweeps * bw, half_cols), f32),
        ],
        axis=0,
    )
    state = state.reshape(-1, pieces, width).transpose(1, 0, 2)

    first_up = lax.ppermute(
        packed[1, 0], "row", [(i + CORES, i) for i in range(0, rows - CORES, CORES)]
    )
    mine = jnp.concatenate(
        [jnp.where(is_low, first_up, packed[1, 0])[None], packed[1, 1:]], axis=0
    )
    mats += list(prep(1, gather(mine)))
    extra_own = [packed[1, 0]] + [
        lax.ppermute(
            packed[1, 0], ("row", "col"), [(i, (i + k) % cols) for i in range(cols)]
        )
        for k in range(1, cols)
    ]
    extra_pair = [lax.ppermute(part, "row", [(0, 1)]) for part in extra_own]
    extra = call(
        functools.partial(prep_extra_kernel, bw, cols),
        [shape(2 * bw, 2 * bw, dtype=bf16)] * 2,
        [jnp.where(is_low, a, b) for a, b in zip(extra_own, extra_pair)],
        scratch=[pltpu.VMEM((bw, 2 * bw), f32)],
        flops=block_flops,
    )

    units = sweeps * pieces
    steps = units + LAG * (chips - 1)
    first_down = (sweeps - 1) * pieces + LAG
    ups, downs = {}, {}
    for step in range(steps):
        working = [
            chip for chip in range(chips) if 0 <= step - LAG * (chips - 1 - chip) < units
        ]
        fresh = 1 if step < pieces else sweeps
        incoming = ups.get(step - LAG)
        if incoming is None:
            incoming = jnp.zeros((bw, width), f32)
        ins = [bounds, state, incoming] + mats[: 2 * fresh]
        if fresh == sweeps:
            ins += list(extra)
        state, up, down = call(
            functools.partial(unit_kernel, step, chips, sweeps, pieces, count, bw, fresh),
            [shape(*state.shape), shape(bw, width), shape(sweeps * bw, width)],
            ins,
            aliases={1: 0},
            smem=(0,),
            flops=3 * 2 * count * 4 * bw * bw * width,
        )
        pairs = [
            (chip * CORES + c, (chip - 1) * CORES + c)
            for chip in working
            if chip > 0
            for c in range(CORES)
        ]
        if pairs:
            ups[step] = lax.ppermute(up, "row", pairs)
        pairs = [
            (chip * CORES + c, (chip + 1) * CORES + c)
            for chip in working
            if chip < chips - 1
            and 0 <= step - LAG * (chips - 1 - chip) - (sweeps - 1) * pieces < pieces
            for c in range(CORES)
        ]
        if pairs:
            downs[step] = lax.ppermute(down, "row", pairs)

    order = sorted(downs)
    half = count * bw // CORES
    keep, give = call(
        functools.partial(finish_kernel, order[0], chips, sweeps, pieces, count, bw),
        [shape(half, half_cols)] * 2,
        [state] + [downs[k] for k in order],
    )
    back = lax.ppermute(give, "row", pair)
    return jnp.concatenate(
        [jnp.where(is_low, keep, back), jnp.where(is_low, back, keep)], axis=1
    )


def solution(mesh):
    placed = (P("row", "col"), P(None, "row", "col", None), P(None, "row", "col", None), P())
    return jax.shard_map(
        per_device, mesh=mesh, in_specs=placed, out_specs=P("row", "col"), check_vma=False
    )
```

```python
import functools

import jax
import jax.numpy as jnp
from jax import lax
from jax.experimental import pallas as pl
from jax.experimental.pallas import tpu as pltpu
from jax.sharding import PartitionSpec as P

LAG = 2
DOWN_LAG = 3
WIDTH = 128
CORES = 2
f32, bf16 = jnp.float32, jnp.bfloat16


def split(x):
    high = x.astype(bf16)
    return high, (x - high.astype(f32)).astype(bf16)


def dot3(a, b, dims):
    (ah, al), (bh, bl) = a, b
    mm = functools.partial(
        lax.dot_general, dimension_numbers=(dims, ((), ())), preferred_element_type=f32
    )
    return mm(ah, bh) + (mm(ah, bl) + mm(al, bh))


def form_block(packed, bw):
    packed_v, factor = packed[:, :bw], packed[:, bw:]
    row = lax.broadcasted_iota(jnp.int32, (bw, bw), 0)
    col = lax.broadcasted_iota(jnp.int32, (bw, bw), 1)
    upper = jnp.where(col >= row, packed_v, 0.0)
    lower = jnp.where(col < row, packed_v, 0.0)
    v = split(jnp.concatenate([upper, lower], axis=1))
    fv = split(dot3(split(factor), v, ((1,), (0,))))
    g = dot3(v, fv, ((0,), (0,)))
    row2 = lax.broadcasted_iota(jnp.int32, (2 * bw, 2 * bw), 0)
    col2 = lax.broadcasted_iota(jnp.int32, (2 * bw, 2 * bw), 1)
    return jnp.where(row2 == col2, 1.0, 0.0) - g


def pack_kernel(bw, reflectors, factors, out):
    for i in range(out.shape[0]):
        out[i, :, :bw] = reflectors[0, i, :, :bw] + reflectors[0, i, :, bw:]
        out[i, :, bw:] = factors[0, i]


def assemble(packed, pieces, index, cols):
    z = lax.axis_index("col")
    part = packed.shape[0] // cols
    for k in range(cols):
        at = lax.rem(z - k + cols, cols) * part
        packed[pl.ds(pl.multiple_of(at, part), part), :] = pieces[k][index]


def prep_kernel(sweep, count, bw, cols, *refs):
    pieces, rest = refs[: 2 * cols], refs[2 * cols :]
    high_ref, low_ref, packed = rest[-3:]
    core = lax.rem(lax.axis_index("row"), CORES)
    local = count // CORES
    if sweep:
        high_ref[: sweep * count] = rest[0][...]
        low_ref[: sweep * count] = rest[1][...]
    for side in range(2):
        owner = core if side == 0 else 1 - core
        for i in range(local):
            assemble(packed, pieces[side * cols : (side + 1) * cols], i, cols)
            slot = sweep * count + lax.rem(owner * local + i - sweep + count, count)
            high, low = split(form_block(packed[...], bw))
            high_ref[slot] = high
            low_ref[slot] = low


def prep_extra_kernel(bw, cols, *refs):
    own, other, (high_ref, low_ref, packed) = refs[:cols], refs[cols : 2 * cols], refs[2 * cols :]
    core = lax.rem(lax.axis_index("row"), CORES)

    @pl.when(core == 0)
    def _():
        assemble(packed, own, slice(None), cols)

    @pl.when(core == 1)
    def _():
        assemble(packed, other, slice(None), cols)

    high, low = split(form_block(packed[...], bw))
    high_ref[...] = high
    low_ref[...] = low


def apply_block(current, high, low, live):
    rh, rl = split(current)
    width = current.shape[1]
    wide = jnp.dot(high, jnp.concatenate([rh, rl], axis=1), preferred_element_type=f32)
    thin = jnp.dot(low, rh, preferred_element_type=f32)
    return jnp.where(live, wide[:, :width] + (wide[:, width:] + thin), current)


def unit_kernel(step, chips, sweeps, pieces, count, bw, has_extra, has_down, *refs):
    bounds, state_in, incoming, high, low = refs[:5]
    rest = refs[5:]
    if has_extra:
        extra_high, extra_low = rest[:2]
        rest = rest[2:]
    state, up = rest[:2]
    chip = lax.axis_index("row") // CORES
    unit = step - LAG * (chips - 1 - chip)
    active = (unit >= 0) & (unit < sweeps * pieces)
    unit = jnp.clip(unit, 0, sweeps * pieces - 1)
    first = 0
    if has_down:
        first = sweeps - 1
    if step < pieces:
        sweep = 0
    elif has_extra:
        sweep = sweeps - 1
    else:
        sweep = unit // pieces
    piece = unit - sweep * pieces

    def live(sweep, block):
        start = block * bw
        return (start >= bounds[sweep, 0]) & (start <= bounds[sweep, 1])

    def at(index, size):
        if isinstance(index, int):
            return slice(index * bw, (index + size) * bw)
        return pl.ds(pl.multiple_of(index * bw, bw), size * bw)

    @pl.when(active)
    def _():
        below = incoming[...]
        for slot in reversed(range(count)):
            rows = state[piece, at(slot + sweep, 1), :]
            current = jnp.concatenate([rows, below], axis=0)
            index = sweep * count + slot
            result = apply_block(
                current, high[index], low[index], live(sweep, chip * count + slot + sweep)
            )
            state[piece, at(slot + sweep + 1, 1), :] = result[bw:]
            below = result[:bw]
        state[piece, at(sweep, 1), :] = below
        up[...] = below
        if has_extra:

            @pl.when((chip == 0) & live(sweep, 0))
            def _():
                current = state[piece, : 2 * bw, :]
                state[piece, : 2 * bw, :] = apply_block(
                    current, extra_high[...], extra_low[...], True
                )

        if has_down:
            rest[2][...] = state[piece, count * bw : (count + sweeps) * bw, :]


def finish_kernel(first_step, chips, sweeps, pieces, count, bw, *refs):
    state, swapped, out = refs[0], refs[1], refs[-1]
    downs = refs[2:-1]
    steps = len(downs) // CORES
    row = lax.axis_index("row")
    chip, core = row // CORES, lax.rem(row, CORES)
    half = count * bw // CORES
    width = state.shape[2]
    for piece in range(pieces):
        near = slice(piece * width, (piece + 1) * width)
        far = slice((pieces + piece) * width, (pieces + piece + 1) * width)

        @pl.when(core == 1)
        def _():
            out[:, near] = swapped[piece]
            out[:, far] = state[piece, half : 2 * half, :]

        @pl.when((core == 0) & (chip == 0))
        def _():
            out[:, near] = state[piece, :half, :]
            out[:, far] = swapped[piece]

        for sender in range(chips - 1):

            @pl.when((core == 0) & (chip == sender + 1))
            def _():
                at = (sweeps - 1) * pieces + piece + LAG * (chips - 1 - sender) - first_step
                out[:, near] = downs[at][...]
                out[:, far] = downs[steps + at][...]


def vmem_spec():
    return pl.BlockSpec(memory_space=pltpu.VMEM)


def call(body, outs, ins, scratch=(), aliases=None, smem=(), flops=0, limit=32):
    specs = [
        pl.BlockSpec(memory_space=pltpu.SMEM) if i in smem else vmem_spec()
        for i in range(len(ins))
    ]
    return pl.pallas_call(
        body,
        out_shape=tuple(outs),
        in_specs=specs,
        out_specs=tuple(vmem_spec() for _ in outs),
        scratch_shapes=list(scratch),
        input_output_aliases=aliases or {},
        cost_estimate=pl.CostEstimate(flops=flops, bytes_accessed=0, transcendentals=0),
        compiler_params=pltpu.CompilerParams(vmem_limit_bytes=limit * 2**20),
    )(*ins)


def pack(reflectors, factors, sweep):
    local, part, bw = factors.shape[1:]
    return pl.pallas_call(
        functools.partial(pack_kernel, bw),
        grid=(1,),
        out_shape=jax.ShapeDtypeStruct((local, part, 2 * bw), f32),
        in_specs=[
            pl.BlockSpec((1, local, part, 2 * bw), lambda i: (sweep, 0, 0, 0)),
            pl.BlockSpec((1, local, part, bw), lambda i: (sweep, 0, 0, 0)),
        ],
        out_specs=pl.BlockSpec((local, part, 2 * bw), lambda i: (0, 0, 0)),
        compiler_params=pltpu.CompilerParams(vmem_limit_bytes=16 * 2**20),
    )(reflectors, factors)


def after(value, *earlier):
    return lax.optimization_barrier((value,) + earlier)[0]


def per_device(vectors, reflectors, factors, bounds):
    rows, cols = lax.axis_size("row"), lax.axis_size("col")
    core = lax.rem(lax.axis_index("row"), CORES)
    is_low = core == 0
    chips = rows // CORES
    row_dev, col_count = vectors.shape
    sweeps, blocks_dev = reflectors.shape[:2]
    bw = reflectors.shape[3] // 2
    count = blocks_dev * CORES
    half = count * bw // CORES
    half_cols = col_count // CORES
    pieces = max(1, half_cols // WIDTH)
    width = half_cols // pieces
    assert sweeps == 2 and blocks_dev == 2

    pair = [(i, i ^ 1) for i in range(rows)]

    def shape(*dims, dtype=f32):
        return jax.ShapeDtypeStruct(dims, dtype)

    def along(x):
        return [x] + [
            lax.ppermute(x, "col", [(i, (i + k) % cols) for i in range(cols)])
            for k in range(1, cols)
        ]

    def across(parts):
        return [lax.ppermute(part, "row", pair) for part in parts]

    block_flops = 3 * 2 * (bw * bw * 2 * bw + 2 * bw * bw * 2 * bw)

    def prep(sweep, parts, earlier=()):
        return call(
            functools.partial(prep_kernel, sweep, count, bw, cols),
            [shape((sweep + 1) * count, 2 * bw, 2 * bw, dtype=bf16)] * 2,
            list(parts) + list(earlier),
            scratch=[pltpu.VMEM((bw, 2 * bw), f32)],
            flops=count * block_flops,
        )

    packed0 = pack(reflectors, factors, 0)
    parts0 = along(packed0)

    vectors = after(vectors, packed0)
    own_part = lax.dynamic_slice_in_dim(vectors, core * half_cols, half_cols, 1)
    other_part = lax.ppermute(
        lax.dynamic_slice_in_dim(vectors, (1 - core) * half_cols, half_cols, 1), "row", pair
    )
    state = jnp.concatenate(
        [
            jnp.where(is_low, own_part, other_part),
            jnp.where(is_low, other_part, own_part),
            jnp.zeros((sweeps * bw, half_cols), f32),
        ],
        axis=0,
    )
    state = state.reshape(-1, pieces, width).transpose(1, 0, 2)
    mats0 = prep(0, parts0 + across(parts0))

    packed1 = pack(after(reflectors, parts0[1]), factors, 1)
    first_up = lax.ppermute(
        packed1[0], "row", [(i + CORES, i) for i in range(0, rows - CORES, CORES)]
    )
    mine = jnp.concatenate(
        [jnp.where(is_low, first_up, packed1[0])[None], packed1[1:]], axis=0
    )
    parts1 = along(mine)
    mats1 = prep(1, parts1 + across(parts1), mats0)
    source = after(packed1[0], parts1[1])
    extra_own = [source] + [
        lax.ppermute(source, ("row", "col"), [(i, (i + k) % cols) for i in range(cols)])
        for k in range(1, cols)
    ]
    extra_other = [lax.ppermute(part, "row", [(0, 1)]) for part in extra_own]
    extra = call(
        functools.partial(prep_extra_kernel, bw, cols),
        [shape(2 * bw, 2 * bw, dtype=bf16)] * 2,
        extra_own + extra_other,
        scratch=[pltpu.VMEM((bw, 2 * bw), f32)],
        flops=block_flops,
    )

    units = sweeps * pieces
    steps = units + LAG * (chips - 1)
    last = (sweeps - 1) * pieces
    ups, downs = {}, {}
    for step in range(steps):
        working = {
            chip: step - LAG * (chips - 1 - chip)
            for chip in range(chips)
            if 0 <= step - LAG * (chips - 1 - chip) < units
        }
        has_extra = all(unit >= last for unit in working.values()) and 0 in working
        senders = [chip for chip in working if chip < chips - 1 and working[chip] >= last]
        incoming = ups.get(step - LAG)
        if incoming is None:
            incoming = jnp.zeros((bw, width), f32)
        if step - DOWN_LAG in downs:
            state, *held = lax.optimization_barrier((state,) + downs[step - DOWN_LAG])
            downs[step - DOWN_LAG] = tuple(held)
        ins = [bounds, state, incoming] + list(mats0 if step < pieces else mats1)
        if has_extra:
            ins += list(extra)
        outs = [shape(*state.shape), shape(bw, width)]
        if senders:
            outs.append(shape(sweeps * bw, width))
        state, up, *down = call(
            functools.partial(
                unit_kernel, step, chips, sweeps, pieces, count, bw, has_extra, bool(senders)
            ),
            outs,
            ins,
            aliases={1: 0},
            smem=(0,),
            flops=3 * 2 * count * 4 * bw * bw * width,
        )
        pairs = [
            (chip * CORES + c, (chip - 1) * CORES + c)
            for chip in working
            if chip > 0
            for c in range(CORES)
        ]
        if pairs:
            ups[step] = lax.ppermute(up, "row", pairs)
        if senders:
            downs[step] = tuple(
                lax.ppermute(
                    down[0],
                    "row",
                    [(chip * CORES + c, (chip + 1) * CORES) for chip in senders],
                )
                for c in range(CORES)
            )

    give = jnp.where(is_low, state[:, half : 2 * half], state[:, :half])
    swapped = lax.ppermute(give, "row", pair)
    order = sorted(downs)
    return call(
        functools.partial(finish_kernel, order[0], chips, sweeps, pieces, count, bw),
        [shape(row_dev, col_count)],
        [state, swapped] + [downs[k][c] for c in range(CORES) for k in order],
    )[0]


def solution(mesh):
    placed = (P("row", "col"), P(None, "row", "col", None), P(None, "row", "col", None), P())
    return jax.shard_map(
        per_device, mesh=mesh, in_specs=placed, out_specs=P("row", "col"), check_vma=False
    )
```

```python
import functools

import jax
import jax.numpy as jnp
from jax import lax
from jax.experimental import pallas as pl
from jax.experimental.pallas import tpu as pltpu
from jax.sharding import PartitionSpec as P

LAG = 2
RELAY_LAG = 2
WIDTH = 128
CORES = 2
LINE = 4
f32, bf16 = jnp.float32, jnp.bfloat16


def split(x):
    high = x.astype(bf16)
    return high, (x - high.astype(f32)).astype(bf16)


def dot3(a, b, dims):
    (ah, al), (bh, bl) = a, b
    mm = functools.partial(
        lax.dot_general, dimension_numbers=(dims, ((), ())), preferred_element_type=f32
    )
    return mm(ah, bh) + (mm(ah, bl) + mm(al, bh))


def form_block(packed, bw):
    packed_v, factor = packed[:, :bw], packed[:, bw:]
    row = lax.broadcasted_iota(jnp.int32, (bw, bw), 0)
    col = lax.broadcasted_iota(jnp.int32, (bw, bw), 1)
    upper = jnp.where(col >= row, packed_v, 0.0)
    lower = jnp.where(col < row, packed_v, 0.0)
    v = split(jnp.concatenate([upper, lower], axis=1))
    fv = split(dot3(split(factor), v, ((1,), (0,))))
    g = dot3(v, fv, ((0,), (0,)))
    row2 = lax.broadcasted_iota(jnp.int32, (2 * bw, 2 * bw), 0)
    col2 = lax.broadcasted_iota(jnp.int32, (2 * bw, 2 * bw), 1)
    return jnp.where(row2 == col2, 1.0, 0.0) - g


def load_kernel(pieces, half_cols, after_ref, vectors, state, give, sems):
    core = lax.rem(lax.axis_index("row"), CORES)
    rows, width = give.shape[1], give.shape[2]
    copies = []
    for piece in range(pieces):
        for side in range(2):
            owner = core if side else 1 - core
            lanes = pl.ds(pl.multiple_of(owner * half_cols + piece * width, width), width)
            into = (
                state.at[piece, pl.ds(pl.multiple_of(core * rows, rows), rows), :]
                if side
                else give.at[piece]
            )
            copies.append(
                pltpu.make_async_copy(vectors.at[:, lanes], into, sems.at[2 * piece + side])
            )
    for copy in copies:
        copy.start()
    for piece in range(pieces):
        state[piece, CORES * rows :, :] = jnp.zeros(
            (state.shape[1] - CORES * rows, width), f32
        )
    for copy in copies:
        copy.wait()


def place_kernel(state_in, taken, state):
    core = lax.rem(lax.axis_index("row"), CORES)
    rows = taken.shape[1]
    for piece in range(taken.shape[0]):
        state[piece, pl.ds(pl.multiple_of((1 - core) * rows, rows), rows), :] = taken[piece]


def pack_kernel(bw, reflectors, factors, out):
    for i in range(out.shape[0]):
        out[i, :, :bw] = reflectors[0, i, :, :bw] + reflectors[0, i, :, bw:]
        out[i, :, bw:] = factors[0, i]


def pack_halves_kernel(bw, after_ref, reflectors, factors, first, second):
    core = lax.rem(lax.axis_index("row"), CORES)
    for i, out in ((1 - core, first), (core, second)):
        out[0, :, :bw] = reflectors[0, i, :, :bw] + reflectors[0, i, :, bw:]
        out[0, :, bw:] = factors[0, i]


def assemble(packed, pieces, index, cols):
    z = lax.axis_index("col")
    part = packed.shape[0] // cols

    def put(source, piece):
        packed[pl.ds(pl.multiple_of(source * part, part), part), :] = piece[index]

    if cols != LINE:
        for k in range(cols):
            put(lax.rem(z - k + cols, cols), pieces[k])
        return
    own, from_low, from_high, from_two, relayed = pieces
    put(z, own)
    put(lax.rem(z + 2, cols), from_two)

    @pl.when(z > 0)
    def _():
        put(z - 1, from_low)

    @pl.when(z < cols - 1)
    def _():
        put(z + 1, from_high)

    @pl.when((z == 0) | (z == cols - 1))
    def _():
        put(cols - 1 - z, relayed)


def form_kernel(bw, cols, used, *refs):
    pieces, out, packed = refs[:used], refs[-2], refs[-1]
    for i in range(out.shape[0]):
        assemble(packed, pieces, i, cols)
        out[i] = form_block(packed[...], bw)


def halves_kernel(slots, aliased, *refs):
    own, other, high_ref, low_ref = refs[0], refs[1], refs[-2], refs[-1]
    core = lax.rem(lax.axis_index("row"), CORES)
    for side, source in ((0, own), (1, other)):
        owner = core if side == 0 else 1 - core
        for i in range(source.shape[0]):
            slot = jnp.where(owner == 0, slots[0][i], slots[1][i])
            high, low = split(source[i])
            high_ref[slot] = high
            low_ref[slot] = low


def extra_kernel(own, other, high_ref, low_ref):
    core = lax.rem(lax.axis_index("row"), CORES)
    high, low = split(jnp.where(core == 0, own[0], other[0]))
    high_ref[...] = high
    low_ref[...] = low


def apply_block(current, high, low, live):
    rh, rl = split(current)
    width = current.shape[1]
    wide = jnp.dot(high, jnp.concatenate([rh, rl], axis=1), preferred_element_type=f32)
    thin = jnp.dot(low, rh, preferred_element_type=f32)
    return jnp.where(live, wide[:, :width] + (wide[:, width:] + thin), current)


def unit_kernel(plan, step, chips, sweeps, pieces, count, bw, *refs):
    bounds, state_in, incoming, high, low = refs[:5]
    rest = refs[5:]
    has_extra, senders, relaying = plan
    if has_extra:
        extra_high, extra_low = rest[:2]
        rest = rest[2:]
    if relaying:
        relay_in = rest[:CORES]
        rest = rest[CORES:]
    state, up = rest[:2]
    down = rest[2:]
    row = lax.axis_index("row")
    chip, core = row // CORES, lax.rem(row, CORES)
    unit = step - LAG * (chips - 1 - chip)
    active = (unit >= 0) & (unit < sweeps * pieces)
    unit = jnp.clip(unit, 0, sweeps * pieces - 1)
    if step < pieces:
        sweep = 0
    elif has_extra:
        sweep = sweeps - 1
    else:
        sweep = unit // pieces
    piece = unit - sweep * pieces

    def live(sweep, block):
        start = block * bw
        return (start >= bounds[sweep, 0]) & (start <= bounds[sweep, 1])

    def at(index, size):
        if isinstance(index, int):
            return slice(index * bw, (index + size) * bw)
        return pl.ds(pl.multiple_of(index * bw, bw), size * bw)

    @pl.when(active)
    def _():
        below = incoming[...]
        for slot in reversed(range(count)):
            rows = state[piece, at(slot + sweep, 1), :]
            current = jnp.concatenate([rows, below], axis=0)
            index = sweep * count + slot
            result = apply_block(
                current, high[index], low[index], live(sweep, chip * count + slot + sweep)
            )
            state[piece, at(slot + sweep + 1, 1), :] = result[bw:]
            below = result[:bw]
        state[piece, at(sweep, 1), :] = below
        up[...] = below
        if has_extra:

            @pl.when((chip == 0) & live(sweep, 0))
            def _():
                current = state[piece, : 2 * bw, :]
                state[piece, : 2 * bw, :] = apply_block(
                    current, extra_high[...], extra_low[...], True
                )

    for sender, done in senders.items():
        for c in range(CORES):

            @pl.when((chip == sender) & (core == c))
            def _():
                down[c][...] = state[done, count * bw : (count + sweeps) * bw, :]

    if relaying:

        @pl.when((chip == chips - 1) & (core == 1))
        def _():
            for c in range(CORES):
                down[c][...] = relay_in[c][...]


def finish_kernel(arrival, chips, pieces, half, *refs):
    state, swapped, out = refs[0], refs[1], refs[-1]
    downs = refs[2:-1]
    steps = len(downs) // CORES
    row = lax.axis_index("row")
    chip, core = row // CORES, lax.rem(row, CORES)
    width = state.shape[2]
    for piece in range(pieces):
        near = slice(piece * width, (piece + 1) * width)
        far = slice((pieces + piece) * width, (pieces + piece + 1) * width)

        @pl.when(core == 1)
        def _():
            out[:, near] = swapped[piece]
            out[:, far] = state[piece, half : 2 * half, :]

        @pl.when((core == 0) & (chip == 0))
        def _():
            out[:, near] = state[piece, :half, :]
            out[:, far] = swapped[piece]

        for sender in range(chips - 1):

            @pl.when((core == 0) & (chip == sender + 1))
            def _():
                at = arrival[sender][piece]
                out[:, near] = downs[at][...]
                out[:, far] = downs[steps + at][...]


def vmem_spec():
    return pl.BlockSpec(memory_space=pltpu.VMEM)


def call(body, outs, ins, scratch=(), aliases=None, special=None, flops=0):
    special = special or {}
    specs = [
        pl.BlockSpec(memory_space=special[i]) if i in special else vmem_spec()
        for i in range(len(ins))
    ]
    return pl.pallas_call(
        body,
        out_shape=tuple(outs),
        in_specs=specs,
        out_specs=tuple(vmem_spec() for _ in outs),
        scratch_shapes=list(scratch),
        input_output_aliases=aliases or {},
        cost_estimate=pl.CostEstimate(flops=flops, bytes_accessed=0, transcendentals=0),
        compiler_params=pltpu.CompilerParams(vmem_limit_bytes=32 * 2**20),
    )(*ins)


def pack(body, reflectors, factors, sweep, out_shapes, earlier=()):
    local, part, bw = factors.shape[1:]
    out_specs = tuple(pl.BlockSpec(out.shape, lambda i: (0, 0, 0)) for out in out_shapes)
    return pl.pallas_call(
        functools.partial(body, bw),
        grid=(1,),
        out_shape=tuple(out_shapes),
        in_specs=[vmem_spec() for _ in earlier]
        + [
            pl.BlockSpec((1, local, part, 2 * bw), lambda i: (sweep, 0, 0, 0)),
            pl.BlockSpec((1, local, part, bw), lambda i: (sweep, 0, 0, 0)),
        ],
        out_specs=out_specs,
        compiler_params=pltpu.CompilerParams(vmem_limit_bytes=16 * 2**20),
    )(*earlier, reflectors, factors)


def gather_col(x, cols):
    if cols != LINE:
        return [x] + [
            lax.ppermute(x, "col", [(i, (i + k) % cols) for i in range(cols)])
            for k in range(1, cols)
        ]
    from_two = lax.ppermute(x, "col", [(i, (i + 2) % cols) for i in range(cols)])
    from_low = lax.ppermute(x, "col", [(i, i + 1) for i in range(cols - 1)])
    from_high = lax.ppermute(x, "col", [(i + 1, i) for i in range(cols - 1)])
    relayed = lax.ppermute(from_two, "col", [(cols - 2, cols - 1), (1, 0)])
    return [x, from_low, from_high, from_two, relayed]


def per_device(vectors, reflectors, factors, bounds):
    rows, cols = lax.axis_size("row"), lax.axis_size("col")
    is_low = lax.rem(lax.axis_index("row"), CORES) == 0
    chips = rows // CORES
    row_dev, col_count = vectors.shape
    sweeps, blocks_dev = reflectors.shape[:2]
    part = reflectors.shape[2]
    bw = reflectors.shape[3] // 2
    count = blocks_dev * CORES
    half = count * bw // CORES
    half_cols = col_count // CORES
    pieces = max(1, half_cols // WIDTH)
    width = half_cols // pieces
    assert sweeps == 2 and blocks_dev == 2

    pair = [(i, i ^ 1) for i in range(rows)]

    def shape(*dims, dtype=f32):
        return jax.ShapeDtypeStruct(dims, dtype)

    block_flops = 3 * 2 * (bw * bw * 2 * bw + 2 * bw * bw * 2 * bw)

    def form(parts, blocks, earlier=()):
        return call(
            functools.partial(form_kernel, bw, cols, len(parts)),
            [shape(blocks, 2 * bw, 2 * bw)],
            list(parts) + list(earlier),
            scratch=[pltpu.VMEM((bw, 2 * bw), f32)],
            flops=blocks * block_flops,
        )[0]

    def to_halves(slots, own, other, before=(), earlier=()):
        return call(
            functools.partial(halves_kernel, slots, bool(before)),
            [shape(sweeps * count, 2 * bw, 2 * bw, dtype=bf16)] * 2,
            [own, other] + list(before) + list(earlier),
            aliases={2: 0, 3: 1} if before else None,
        )

    packed0 = pack(pack_kernel, reflectors, factors, 0, [shape(blocks_dev, part, 2 * bw)])[0]
    parts0 = gather_col(packed0, cols)

    state, give = call(
        functools.partial(load_kernel, pieces, half_cols),
        [shape(pieces, (count + sweeps) * bw, width), shape(pieces, row_dev, width)],
        [packed0, vectors],
        scratch=[pltpu.SemaphoreType.DMA((2 * pieces,))],
        special={1: pl.ANY},
    )
    state = call(
        place_kernel, [shape(*state.shape)], [state, lax.ppermute(give, "row", pair)], aliases={0: 0}
    )[0]

    first, second = pack(
        pack_halves_kernel,
        reflectors,
        factors,
        1,
        [shape(1, part, 2 * bw)] * 2,
        earlier=[parts0[-2]],
    )
    parts1 = gather_col(first, cols)
    first_up = lax.ppermute(
        second, "row", [(i + CORES, i) for i in range(0, rows - CORES, CORES)]
    )

    own0 = form(parts0, blocks_dev, [state])
    mats = to_halves(((0, 1), (2, 3)), own0, lax.ppermute(own0, "row", pair))

    parts2 = gather_col(lax.optimization_barrier((jnp.where(is_low, first_up, second), parts1[-2]))[0], cols)
    own1 = form(parts1, 1)
    other1 = lax.ppermute(own1, "row", pair)
    own2 = form(parts2, 1)
    other2 = lax.ppermute(own2, "row", pair)

    source = lax.optimization_barrier((second, parts2[-2]))[0]
    if cols != LINE:
        extra_parts = [source] + [
            lax.ppermute(source, ("row", "col"), [(i, (i + k) % cols) for i in range(cols)])
            for k in range(1, cols)
        ]
    else:
        two = lax.ppermute(source, ("row", "col"), [(i, (i + 2) % cols) for i in range(cols)])
        extra_parts = [
            source,
            lax.ppermute(source, ("row", "col"), [(i, i + 1) for i in range(cols - 1)]),
            lax.ppermute(source, ("row", "col"), [(i + 1, i) for i in range(cols - 1)]),
            two,
            lax.ppermute(two, ("row", "col"), [(cols - 2, cols - 1), (1, 0)]),
        ]
    own3 = form(extra_parts, 1)
    extra = call(
        extra_kernel,
        [shape(2 * bw, 2 * bw, dtype=bf16)] * 2,
        [own3, lax.ppermute(own3, "row", [(0, 1)])],
    )

    units = sweeps * pieces
    steps = units + LAG * (chips - 1)
    last = (sweeps - 1) * pieces

    def relayed(chip):
        return chip % 2 == 1 and chip + 2 == chips - 1

    def delay(chip):
        return min(pieces, LAG * chip) if chip % 2 == 0 else 0

    def sent(chip, piece):
        return piece + last + LAG * (chips - 1 - chip) + delay(chip)

    ups, downs = {}, {}
    for step in range(steps):
        working = {
            chip: step - LAG * (chips - 1 - chip)
            for chip in range(chips)
            if 0 <= step - LAG * (chips - 1 - chip) < units
        }
        has_extra = all(unit >= last for unit in working.values()) and 0 in working
        senders = {
            chip: piece
            for chip in range(chips - 1)
            for piece in range(pieces)
            if sent(chip, piece) == step
        }
        relaying = any(
            relayed(chip) and sent(chip, piece) + RELAY_LAG == step
            for chip in range(chips - 1)
            for piece in range(pieces)
        )
        if step == pieces:
            mats = to_halves(((count,), (count + 1,)), own1, other1, mats, [up])
        if step == pieces + LAG:
            mats = to_halves(((2 * count - 1,), (count + 2,)), own2, other2, mats, [up])
        mats = list(mats)
        incoming = ups.get(step - LAG)
        if incoming is None:
            incoming = jnp.zeros((bw, width), f32)
        ins = [bounds, state, incoming] + mats
        if has_extra:
            ins += list(extra)
        if relaying:
            ins += list(downs[step - RELAY_LAG])
        outs = [shape(*state.shape), shape(bw, width)]
        if senders or relaying:
            outs += [shape(sweeps * bw, width)] * CORES
        state, up, *down = call(
            functools.partial(
                unit_kernel, (has_extra, senders, relaying), step, chips, sweeps, pieces, count, bw
            ),
            outs,
            ins,
            aliases={1: 0},
            special={0: pltpu.SMEM},
            flops=3 * 2 * count * 4 * bw * bw * width,
        )
        pairs = [
            (chip * CORES + c, (chip - 1) * CORES + c)
            for chip in working
            if chip > 0
            for c in range(CORES)
        ]
        if pairs:
            ups[step] = lax.ppermute(up, "row", pairs)
        if senders or relaying:
            moves = []
            for c in range(CORES):
                pairs = []
                for chip in senders:
                    target = (chip + 2) * CORES + 1 if relayed(chip) else (chip + 1) * CORES
                    pairs.append((chip * CORES + c, target))
                if relaying:
                    pairs.append((rows - 1, (chips - 2) * CORES))
                moves.append(lax.ppermute(down[c], "row", pairs))
            downs[step] = tuple(moves)

    give = jnp.where(is_low, state[:, half : 2 * half], state[:, :half])
    swapped = lax.ppermute(give, "row", pair)
    order = sorted(downs)
    arrival = [
        [
            order.index(sent(chip, piece) + (RELAY_LAG if relayed(chip) else 0))
            for piece in range(pieces)
        ]
        for chip in range(chips - 1)
    ]
    return call(
        functools.partial(finish_kernel, arrival, chips, pieces, half),
        [shape(row_dev, col_count)],
        [state, swapped] + [downs[k][c] for c in range(CORES) for k in order],
    )[0]


def solution(mesh):
    placed = (P("row", "col"), P(None, "row", "col", None), P(None, "row", "col", None), P())
    return jax.shard_map(
        per_device, mesh=mesh, in_specs=placed, out_specs=P("row", "col"), check_vma=False
    )
```
